128 devices in a mesh: dp: 2 (over core), ep: 64 (over x, y, z).
Axes of the slice: x: 4, y: 4, z: 4, core: 2. Of those that a mesh axis runs over, the one named last changes fastest.
Arguments:
- x: bfloat16 [2, 64, 256, 1792], P('dp', 'ep'), parts along dimension 0
- expert: int32 [2, 64, 256, 8], P('dp', 'ep'), parts along dimension 0
- slot: int32 [2, 64, 256, 8], P('dp', 'ep'), parts along dimension 0
- gate: float32 [2, 64, 256, 8], P('dp', 'ep'), parts along dimension 0
- w_gate: bfloat16 [128, 1792, 2048], P('ep')
- w_up: bfloat16 [128, 1792, 2048], P('ep')
- w_down: bfloat16 [128, 2048, 1792], P('ep')
- s_gate: bfloat16 [1792, 2048], replicated
- s_up: bfloat16 [1792, 2048], replicated
- s_down: bfloat16 [2048, 1792], replicated
Outputs:
- y: bfloat16 [2, 64, 256, 1792], P('dp', 'ep'), parts along dimension 0
There are 2 independent parts. The reference program is written for one: setup_inputs(seed, part) draws one part's arguments, and reference() takes and returns one part's arrays. A program takes and returns all parts, laid end to end along the dimension named above; an argument that names none is the same for every part.
All inputs are finite; a program needn't handle non-finite values.
Results may differ from the reference program's by a relative error of at most 0.009.
Values are sent between devices in bfloat16 or wider.
A program may use at most 1.5 GiB of HBM per device.

```python
import jax
import jax.numpy as jnp

MEMBERS = 64
TOKENS = 256
D = 1792
FF = 2048
TOP = 8
EXPERTS = 128
SHARED_FF = 2048
SLOTS = 5 * TOKENS * TOP // (4 * EXPERTS)


def setup_inputs(seed: int = 0, part: int = 0) -> dict:
    own, k1, k2, k3, k4, k5, k6 = jax.random.split(jax.random.key(seed), 7)
    kx, ke, kl, kg = jax.random.split(jax.random.fold_in(own, part), 4)
    devices = (1, MEMBERS)
    place = jax.random.permutation(kl, jnp.arange(EXPERTS, dtype=jnp.uint32))
    slow = ((EXPERTS + (9 * place) % EXPERTS) << ((9 * place) // EXPERTS)) // EXPERTS
    wait = (jax.random.bits(ke, (*devices, TOKENS, EXPERTS), jnp.uint32) >> 10) * slow
    expert = jnp.argsort(wait, axis=-1)[..., :TOP].astype(jnp.int32)
    chosen = jax.nn.one_hot(expert, EXPERTS, dtype=jnp.int32)
    in_line = jnp.cumsum(chosen.reshape(*devices, TOKENS * TOP, EXPERTS), axis=2) - 1
    slot = jnp.sum(in_line.reshape(chosen.shape) * chosen, axis=-1)

    def one(key, rows, columns):
        return (jax.random.normal(key, (rows, columns), jnp.float32) * rows**-0.5).astype(jnp.bfloat16)

    def weights(key, rows, columns):
        return jax.lax.map(lambda k: one(k, rows, columns), jax.random.split(key, EXPERTS))

    return {
        "x": jax.random.normal(kx, (*devices, TOKENS, D), jnp.float32).astype(jnp.bfloat16),
        "expert": expert,
        "slot": slot,
        "gate": jax.nn.softmax(jax.random.normal(kg, expert.shape, jnp.float32)),
        "w_gate": weights(k1, D, FF),
        "w_up": weights(k2, D, FF),
        "w_down": weights(k3, FF, D),
        "s_gate": one(k4, D, SHARED_FF),
        "s_up": one(k5, D, SHARED_FF),
        "s_down": one(k6, SHARED_FF, D),
    }


def einsum(form, a, b):
    return jnp.einsum(form, a.astype(jnp.float32), b.astype(jnp.float32))


def for_all(x, s_gate, s_up, s_down):
    h = jax.nn.silu(einsum("...d,df->...f", x, s_gate)) * einsum("...d,df->...f", x, s_up)
    return einsum("...f,fd->...d", h.astype(jnp.bfloat16), s_down)


def reference(x, expert, slot, gate, w_gate, w_up, w_down, s_gate, s_up, s_down):
    to_expert = jax.nn.one_hot(expert, EXPERTS, dtype=jnp.bfloat16)
    to_slot = jax.nn.one_hot(slot, SLOTS, dtype=jnp.bfloat16)
    weighted = to_expert * gate[..., None].astype(jnp.bfloat16)
    dispatch = einsum("abtke,abtkc->abtec", to_expert, to_slot).astype(jnp.bfloat16)
    combine = einsum("abtke,abtkc->abtec", weighted, to_slot).astype(jnp.bfloat16)
    z = einsum("abtec,abtd->aebcd", dispatch, x).astype(jnp.bfloat16)
    h = jax.nn.silu(einsum("aebcd,edf->aebcf", z, w_gate))
    h = (h * einsum("aebcd,edf->aebcf", z, w_up)).astype(jnp.bfloat16)
    out = einsum("aebcf,efd->aebcd", h, w_down).astype(jnp.bfloat16)
    y = einsum("abtec,aebcd->abtd", combine, out)
    return (y + for_all(x, s_gate, s_up, s_down)).astype(jnp.bfloat16)
```

```python
import jax
import jax.numpy as jnp
from jax import lax
from jax.experimental import pallas as pl
from jax.experimental.pallas import tpu as pltpu
from jax.sharding import PartitionSpec as P

F32, BF16 = jnp.float32, jnp.bfloat16
T, D, FF, TOP, SLOTS = 256, 1792, 2048, 8, 20
GROUPS = 5
TILE = 256
STEPS = FF // TILE
BUFS = 3
LANES = ((0, 640), (640, 640), (1280, 512))
OTHERS = ((1, 2), (0, 2), (0, 1))
MESH = pl.DeviceIdType.MESH
OFFSETS = tuple((a, b) for a in range(4) for b in range(4) if (a, b) != (0, 0))


def part(p):
    return pl.ds(*LANES[p])


def contract_rows(a, b):
    return lax.dot_general(a, b, (((0,), (0,)), ((), ())), preferred_element_type=F32)


def dot(a, b):
    return jnp.dot(a, b, preferred_element_type=F32)


def kernel(x, expert, slot, gate, wg, wu, wd, sg, su, sd, y,
           lines, mine, tables, out_rows, z, back, acc, total, last, bg, bu, bd,
           s1, r1, st, rt, sz, rz, sc, rc, sl, rl, wsem):
    me = lax.axis_index("ep")
    coord = (me // 16, (me // 4) % 4, me % 4)

    def moved(p, by):
        c = list(coord)
        c[p] = (c[p] + by) % 4
        return c

    def device(c):
        return {"ep": c[0] * 16 + c[1] * 4 + c[2]}

    def send(src, dst, ss, rs, c):
        pltpu.make_async_remote_copy(src_ref=src, dst_ref=dst, send_sem=ss, recv_sem=rs,
                                     device_id=device(c), device_id_type=MESH).start()

    def wait(like, sem):
        pltpu.make_async_copy(like, like, sem).wait()

    def in_plane(p, c):
        return c[OTHERS[p][0]] * 4 + c[OTHERS[p][1]]

    def rows_of(p, g, c):
        at = [g, *c, slice(None), part(p)]
        at[1 + p] = slice(None)
        return tuple(at)

    def weights(n):
        b = n % BUFS

        @pl.when(n < STEPS)
        def _():
            f = pl.multiple_of(n * TILE, TILE)
            pltpu.make_async_copy(sg.at[:, pl.ds(f, TILE)], bg.at[b], wsem.at[b, 0]).start()
            pltpu.make_async_copy(su.at[:, pl.ds(f, TILE)], bu.at[b], wsem.at[b, 1]).start()
            pltpu.make_async_copy(sd.at[pl.ds(f, TILE), :], bd.at[b], wsem.at[b, 2]).start()

        @pl.when((n >= STEPS) & (n < 7 * STEPS))
        def _():
            e = (n - STEPS) // (3 * STEPS)
            f = pl.multiple_of((n % STEPS) * TILE, TILE)
            pltpu.make_async_copy(wg.at[e, :, pl.ds(f, TILE)], bg.at[b], wsem.at[b, 0]).start()
            pltpu.make_async_copy(wu.at[e, :, pl.ds(f, TILE)], bu.at[b], wsem.at[b, 1]).start()
            pltpu.make_async_copy(wd.at[e, pl.ds(f, TILE), :], bd.at[b], wsem.at[b, 2]).start()

    def ready(n):
        b = n % BUFS
        wait(bg.at[b], wsem.at[b, 0])
        wait(bu.at[b], wsem.at[b, 1])
        wait(bd.at[b], wsem.at[b, 2])
        return b

    weights(0)
    weights(1)
    for by in (2, 1, 3):
        for p in range(3):
            send(x.at[:, part(p)], lines.at[coord[p], :, part(p)], s1.at[p], r1.at[p], moved(p, by))
    for p in range(3):
        lines[coord[p], :, part(p)] = x[:, part(p)]

    ex, sl_ = expert[...], slot[...]
    dev, at = ex >> 1, (ex & 1) * SLOTS + sl_
    valid = sl_ < SLOTS
    c = (dev >> 4, (dev >> 2) & 3, dev & 3)
    g8, j8 = at >> 3, at & 7
    gates = gate[...].astype(BF16).astype(F32)
    number = lax.broadcasted_iota(jnp.int32, (T, 128), 0).astype(F32) + 1.0
    lane = lax.broadcasted_iota(jnp.int32, (T, 128), 1)
    for p in range(3):
        row = jnp.where(valid, c[p] * 8 + g8, -1)
        col = (c[OTHERS[p][0]] * 4 + c[OTHERS[p][1]]) * 8 + j8
        table = jnp.zeros((128, 256), F32)
        for k in range(TOP):
            left = (lane == row[:, k:k + 1]).astype(BF16)
            here = lane == col[:, k:k + 1]
            right = jnp.concatenate([jnp.where(here, number, 0.0), jnp.where(here, gates[:, k:k + 1], 0.0)], axis=1)
            table += contract_rows(left, right.astype(BF16))
        for i in range(4):
            mine[p, i, 0:8, :] = table[8 * i:8 * i + 8, :128]
            mine[p, i, 8:16, :] = table[8 * i:8 * i + 8, 128:]
        tables[p, coord[p]] = mine[p, coord[p]]
    for by in (2, 1, 3):
        for p in range(3):
            to = moved(p, by)
            send(mine.at[p, to[p]], tables.at[p, coord[p]], st.at[p], rt.at[p], to)

    total[...] = jnp.zeros_like(total)

    def shared(n, _):
        weights(n + 2)
        b = ready(n)
        h = jax.nn.silu(dot(x[...], bg[b])) * dot(x[...], bu[b])
        total[...] += dot(h.astype(BF16), bd[b])
        return 0

    lax.fori_loop(0, STEPS, shared, 0)
    for p in range(3):
        wait(lines.at[0:3, :, part(p)], r1.at[p])
        wait(tables.at[p, 0:3], rt.at[p])

    def dispatch(g):
        for p in range(3):
            for i in range(4):
                pick = (number == tables[p, i, pl.ds(g, 1), :]).astype(BF16)
                rows = contract_rows(pick, lines[i, :, part(p)]).astype(BF16)
                out_rows[g, i, :, :, part(p)] = rows.reshape(16, 8, LANES[p][1])
        for a, b in OFFSETS:
            for p in range(3):
                to = list(coord)
                to[OTHERS[p][0]] = (to[OTHERS[p][0]] + a) % 4
                to[OTHERS[p][1]] = (to[OTHERS[p][1]] + b) % 4
                send(out_rows.at[g, :, in_plane(p, to), :, part(p)], z.at[rows_of(p, g, coord)],
                     sz.at[g], rz.at[g], to)
        for p in range(3):
            z[rows_of(p, g, coord)] = out_rows[g, :, in_plane(p, coord), :, part(p)]

    def give_back(g):
        for a, b in OFFSETS:
            for p in range(3):
                to = list(coord)
                to[OTHERS[p][0]] = (to[OTHERS[p][0]] + a) % 4
                to[OTHERS[p][1]] = (to[OTHERS[p][1]] + b) % 4
                send(z.at[rows_of(p, g, to)], back.at[:, g, in_plane(p, coord), :, part(p)],
                     sc.at[g], rc.at[g], to)
        for p in range(3):
            back[:, g, in_plane(p, coord), :, part(p)] = z[rows_of(p, g, coord)]

    def experts(i):
        e = i // 3
        g = i - e

        @pl.when(i != 3)
        def _():
            wait(out_rows.at[g, :, 0:15], rz.at[g])
            acc[...] = jnp.zeros_like(acc)

        at = g * 8 + (lax.broadcasted_iota(jnp.int32, (512, TILE), 0) & 7)
        own = (at >= SLOTS) == (e == 1)

        def step(f, _):
            n = STEPS + i * STEPS + f
            weights(n + 2)
            b = ready(n)
            rows = z[g].reshape(512, D)
            h = jax.nn.silu(dot(rows, bg[b])) * dot(rows, bu[b])
            acc[...] += dot(jnp.where(own, h, 0.0).astype(BF16), bd[b])
            return 0

        lax.fori_loop(0, STEPS, step, 0)

        @pl.when(i != 2)
        def _():
            z[g] = acc[...].astype(BF16).reshape(4, 4, 4, 8, D)
            give_back(g)

    def turn(u, _):
        @pl.when(u < GROUPS)
        def _():
            dispatch(u)

        @pl.when(u >= 2)
        def _():
            experts(u - 2)

        return 0

    lax.fori_loop(0, 8, turn, 0)

    for g in range(GROUPS):
        wait(back.at[:, g, 0:15], rc.at[g])
    for by in (2, 1, 3, 0):
        for p in range(3):
            to = moved(p, by)
            i = to[p]
            mix = jnp.concatenate(
                [jnp.where(number == tables[p, i, g:g + 1, :], tables[p, i, 8 + g:9 + g, :], 0.0).astype(BF16)
                 for g in range(GROUPS)], axis=1)
            summed = dot(mix, back[i, :, :, :, part(p)].reshape(GROUPS * 128, LANES[p][1]))
            if by:
                lines[i, :, part(p)] = summed.astype(BF16)
                send(lines.at[i, :, part(p)], last.at[coord[p], :, part(p)], sl.at[p], rl.at[p], to)
            else:
                total[:, part(p)] += summed
    for p in range(3):
        wait(last.at[0:3, :, part(p)], rl.at[p])
        for by in (1, 2, 3):
            total[:, part(p)] += last[moved(p, by)[p], :, part(p)].astype(F32)
    y[...] = total[...].astype(BF16)

    for p in range(3):
        wait(lines.at[0:3, :, part(p)], s1.at[p])
        wait(tables.at[p, 0:3], st.at[p])
        wait(last.at[0:3, :, part(p)], sl.at[p])
    for g in range(GROUPS):
        wait(out_rows.at[g, :, 0:15], sz.at[g])
        wait(back.at[:, g, 0:15], sc.at[g])


def solution(mesh):
    dma = pltpu.SemaphoreType.DMA

    def body(x, expert, slot, gate, wg, wu, wd, sg, su, sd):
        vmem, anywhere = pl.BlockSpec(memory_space=pltpu.VMEM), pl.BlockSpec(memory_space=pl.ANY)
        out = pl.pallas_call(
            kernel,
            out_shape=jax.ShapeDtypeStruct((T, D), BF16),
            in_specs=[vmem] * 4 + [anywhere] * 6,
            out_specs=vmem,
            scratch_shapes=[
                pltpu.VMEM((4, T, D), BF16),
                pltpu.VMEM((3, 4, 16, 128), F32),
                pltpu.VMEM((3, 4, 16, 128), F32),
                pltpu.VMEM((GROUPS, 4, 16, 8, D), BF16),
                pltpu.VMEM((GROUPS, 4, 4, 4, 8, D), BF16),
                pltpu.VMEM((4, GROUPS, 16, 8, D), BF16),
                pltpu.VMEM((512, D), F32),
                pltpu.VMEM((T, D), F32),
                pltpu.VMEM((4, T, D), BF16),
                pltpu.VMEM((BUFS, D, TILE), BF16),
                pltpu.VMEM((BUFS, D, TILE), BF16),
                pltpu.VMEM((BUFS, TILE, D), BF16),
                dma((3,)), dma((3,)), dma((3,)), dma((3,)),
                dma((GROUPS,)), dma((GROUPS,)), dma((GROUPS,)), dma((GROUPS,)),
                dma((3,)), dma((3,)), dma((BUFS, 3)),
            ],
            compiler_params=pltpu.CompilerParams(has_side_effects=True, vmem_limit_bytes=67043328),
            name="moe",
        )(x[0, 0], expert[0, 0], slot[0, 0], gate[0, 0], wg, wu, wd, sg, su, sd)
        return out[None, None]

    tokens, experts = P("dp", "ep", None, None), P("ep", None, None)
    return jax.shard_map(body, mesh=mesh, in_specs=(tokens,) * 4 + (experts,) * 3 + (P(None, None),) * 3,
                         out_specs=tokens, check_vma=False)
```

```python
import jax
import jax.numpy as jnp
from jax import lax
from jax.experimental import pallas as pl
from jax.experimental.pallas import tpu as pltpu
from jax.sharding import PartitionSpec as P

F32, BF16 = jnp.float32, jnp.bfloat16
T, D, FF, TOP, SLOTS = 256, 1792, 2048, 8, 20
GROUPS = 5
TILE = 256
STEPS = FF // TILE
BUFS = 3
LANES = ((0, 640), (640, 640), (1280, 512))
OTHERS = ((1, 2), (0, 2), (0, 1))
HALF = (slice(0, T // 2), slice(T // 2, T))
TO_NEXT = ((1, 0), (3, 1), (1, 1), (3, 0))
PASS_ON = 5
MESH = pl.DeviceIdType.MESH
NEAR = tuple((a, b, c) for a in range(4) for b in range(4) for c in range(4) if 0 in (a, b, c) and (a, b, c) != (0, 0, 0))
OFFSETS = tuple((a, b) for a in range(4) for b in range(4) if (a, b) != (0, 0))


def part(p):
    return pl.ds(*LANES[p])


def contract_rows(a, b):
    return lax.dot_general(a, b, (((0,), (0,)), ((), ())), preferred_element_type=F32)


def dot(a, b):
    return jnp.dot(a, b, preferred_element_type=F32)


def kernel(x, expert, slot, gate, wg, wu, wd, sg, su, sd, y,
           lines, mine, tables, out_rows, z, back, acc, total, hop, last, bg, bu, bd,
           s1, r1, st, rt, sz, rz, sc, rc, sl, rl, wsem):
    me, swap = lax.axis_index("ep"), lax.axis_index("dp") == 1

    def coordinates(d):
        u, v, w = d >> 4, (d >> 2) & 3, d & 3
        return u, jnp.where(swap, w, v), jnp.where(swap, v, w)

    coord = coordinates(me)

    def moved(p, by):
        c = list(coord)
        c[p] = (c[p] + by) % 4
        return c

    def device(c):
        return {"ep": c[0] * 16 + jnp.where(swap, c[2] * 4 + c[1], c[1] * 4 + c[2])}

    def send(src, dst, ss, rs, c):
        pltpu.make_async_remote_copy(src_ref=src, dst_ref=dst, send_sem=ss, recv_sem=rs,
                                     device_id=device(c), device_id_type=MESH).start()

    def wait(like, sem):
        pltpu.make_async_copy(like, like, sem).wait()

    def in_plane(p, c):
        return c[OTHERS[p][0]] * 4 + c[OTHERS[p][1]]

    def rows_of(p, g, c):
        at = [g, *c, slice(None), part(p)]
        at[1 + p] = slice(None)
        return tuple(at)

    def weights(n):
        b = n % BUFS

        @pl.when(n < STEPS)
        def _():
            f = pl.multiple_of(n * TILE, TILE)
            pltpu.make_async_copy(sg.at[:, pl.ds(f, TILE)], bg.at[b], wsem.at[b, 0]).start()
            pltpu.make_async_copy(su.at[:, pl.ds(f, TILE)], bu.at[b], wsem.at[b, 1]).start()
            pltpu.make_async_copy(sd.at[pl.ds(f, TILE), :], bd.at[b], wsem.at[b, 2]).start()

        @pl.when((n >= STEPS) & (n < 7 * STEPS))
        def _():
            e = (n - STEPS) // (3 * STEPS)
            f = pl.multiple_of((n % STEPS) * TILE, TILE)
            pltpu.make_async_copy(wg.at[e, :, pl.ds(f, TILE)], bg.at[b], wsem.at[b, 0]).start()
            pltpu.make_async_copy(wu.at[e, :, pl.ds(f, TILE)], bu.at[b], wsem.at[b, 1]).start()
            pltpu.make_async_copy(wd.at[e, pl.ds(f, TILE), :], bd.at[b], wsem.at[b, 2]).start()

    def ready(n):
        b = n % BUFS
        wait(bg.at[b], wsem.at[b, 0])
        wait(bu.at[b], wsem.at[b, 1])
        wait(bd.at[b], wsem.at[b, 2])
        return b

    entered = pltpu.get_barrier_semaphore()
    for by in NEAR:
        to = [(v + d) % 4 for v, d in zip(coord, by)]
        pl.semaphore_signal(entered, inc=1, device_id=device(to), device_id_type=MESH)
    weights(0)
    weights(1)

    ex, sl_ = expert[...], slot[...]
    c, at = coordinates(ex >> 1), (ex & 1) * SLOTS + sl_
    valid = sl_ < SLOTS
    g8, j8 = at >> 3, at & 7
    gates = gate[...].astype(BF16).astype(F32)
    along = lax.broadcasted_iota(jnp.int32, (128, T), 1).astype(F32) + 1.0
    down = lax.broadcasted_iota(jnp.int32, (128, T), 0)
    for p in range(3):
        row = jnp.where(valid, c[p] * 8 + g8, -1)
        col = (c[OTHERS[p][0]] * 4 + c[OTHERS[p][1]]) * 8 + j8
        table = jnp.zeros((32, 256), F32)
        for k in range(TOP):
            left = (down[:32] == row[k:k + 1, :]).astype(BF16)
            here = down == col[k:k + 1, :]
            right = jnp.concatenate([jnp.where(here, along, 0.0), jnp.where(here, gates[k:k + 1, :], 0.0)], axis=0)
            table += lax.dot_general(left, right.astype(BF16), (((1,), (1,)), ((), ())), preferred_element_type=F32)
        for i in range(4):
            mine[p, i, 0:8, :] = table[8 * i:8 * i + 8, :128]
            mine[p, i, 8:16, :] = table[8 * i:8 * i + 8, 128:]
        tables[p, coord[p]] = mine[p, coord[p]]
    number = lax.broadcasted_iota(jnp.int32, (T, 128), 0).astype(F32) + 1.0
    pl.semaphore_wait(entered, len(NEAR))

    for by in (2, 1, 3):
        for p in range(3):
            to = moved(p, by)
            send(mine.at[p, to[p]], tables.at[p, coord[p]], st.at[p], rt.at[p], to)
    for first, half in ((1, 0), (3, 1), (1, 1), (3, 0)):
        for p in range(3):
            k = TO_NEXT.index((first, half))
            send(x.at[HALF[half], part(p)], lines.at[coord[p], HALF[half], part(p)],
                 s1.at[p, k], r1.at[p, k], moved(p, first))
    for p in range(3):
        lines[coord[p], :, part(p)] = x[:, part(p)]

    total[...] = jnp.zeros_like(total)

    def pass_on():
        for k, (first, half) in enumerate(TO_NEXT[:2]):
            for p in range(3):
                i = moved(p, 4 - first)[p]
                arrived = lines.at[i, HALF[half], part(p)]
                wait(arrived, r1.at[p, k])
                send(arrived, arrived, s1.at[p, 4 + k], r1.at[p, 4 + k], moved(p, first))

    def shared(n, _):
        @pl.when(n == PASS_ON)
        def _():
            pass_on()

        weights(n + 2)
        b = ready(n)
        h = jax.nn.silu(dot(x[...], bg[b])) * dot(x[...], bu[b])
        total[...] += dot(h.astype(BF16), bd[b])
        return 0

    lax.fori_loop(0, STEPS, shared, 0)
    for p in range(3):
        for k in range(2, 6):
            wait(lines.at[0, HALF[0], part(p)], r1.at[p, k])
        wait(tables.at[p, 0:3], rt.at[p])

    def dispatch(g):
        for p in range(3):
            for i in range(4):
                pick = (number == tables[p, i, pl.ds(g, 1), :]).astype(BF16)
                rows = contract_rows(pick, lines[i, :, part(p)]).astype(BF16)
                out_rows[g, i, :, :, part(p)] = rows.reshape(16, 8, LANES[p][1])
            for a, b in OFFSETS:
                to = list(coord)
                to[OTHERS[p][0]] = (to[OTHERS[p][0]] + a) % 4
                to[OTHERS[p][1]] = (to[OTHERS[p][1]] + b) % 4
                send(out_rows.at[g, :, in_plane(p, to), :, part(p)], z.at[rows_of(p, g, coord)],
                     sz.at[g], rz.at[g], to)
        for p in range(3):
            z[rows_of(p, g, coord)] = out_rows[g, :, in_plane(p, coord), :, part(p)]

    def give_back(g):
        for a, b in OFFSETS:
            for p in range(3):
                to = list(coord)
                to[OTHERS[p][0]] = (to[OTHERS[p][0]] + a) % 4
                to[OTHERS[p][1]] = (to[OTHERS[p][1]] + b) % 4
                send(z.at[rows_of(p, g, to)], back.at[:, g, in_plane(p, coord), :, part(p)],
                     sc.at[g], rc.at[g], to)
        for p in range(3):
            back[:, g, in_plane(p, coord), :, part(p)] = z[rows_of(p, g, coord)]

    def experts(i):
        e = i // 3
        g = i - e

        @pl.when(i != 3)
        def _():
            wait(out_rows.at[g, :, 0:15], rz.at[g])
            acc[...] = jnp.zeros_like(acc)

        at = g * 8 + (lax.broadcasted_iota(jnp.int32, (512, TILE), 0) & 7)
        own = (at >= SLOTS) == (e == 1)

        def step(f, _):
            n = STEPS + i * STEPS + f
            weights(n + 2)
            b = ready(n)
            rows = z[g].reshape(512, D)
            h = jax.nn.silu(dot(rows, bg[b])) * dot(rows, bu[b])
            acc[...] += dot(jnp.where(own, h, 0.0).astype(BF16), bd[b])
            return 0

        lax.fori_loop(0, STEPS, step, 0)

        @pl.when(i != 2)
        def _():
            z[g] = acc[...].astype(BF16).reshape(4, 4, 4, 8, D)
            give_back(g)

    def turn(u, _):
        @pl.when(u < GROUPS)
        def _():
            dispatch(u)

        @pl.when(u >= 2)
        def _():
            experts(u - 2)

        return 0

    lax.fori_loop(0, 8, turn, 0)

    for g in range(GROUPS):
        wait(back.at[:, g, 0:15], rc.at[g])
    def summed(p, i):
        mix = jnp.concatenate(
            [jnp.where(number == tables[p, i, g:g + 1, :], tables[p, i, 8 + g:9 + g, :], 0.0).astype(BF16)
             for g in range(GROUPS)], axis=1)
        return dot(mix, back[i, :, :, :, part(p)].reshape(GROUPS * 128, LANES[p][1]))

    for p in range(3):
        for k in range(2):
            wait(lines.at[0, HALF[0], part(p)], s1.at[p, 4 + k])
    for p in range(3):
        i = moved(p, 2)[p]
        lines[i, :, part(p)] = summed(p, i).astype(BF16)
        for k, by in enumerate((3, 1)):
            send(lines.at[i, HALF[k], part(p)], hop.at[k, :, part(p)], sl.at[p, k], rl.at[p, k], moved(p, by))
    for k, by in enumerate((3, 1)):
        for p in range(3):
            to = moved(p, by)
            own = summed(p, to[p])
            lines[to[p], HALF[1 - k], part(p)] = own[HALF[1 - k]].astype(BF16)
            send(lines.at[to[p], HALF[1 - k], part(p)], last.at[k, HALF[1 - k], part(p)],
                 sl.at[p, 2 + k], rl.at[p, 2 + k], to)
            acc[HALF[k], part(p)] = own[HALF[k]]
    for k, by in enumerate((3, 1)):
        for p in range(3):
            to = moved(p, by)
            wait(hop.at[k, :, part(p)], rl.at[p, k])
            both = acc[HALF[k], part(p)] + hop[k, :, part(p)].astype(F32)
            lines[to[p], HALF[k], part(p)] = both.astype(BF16)
            send(lines.at[to[p], HALF[k], part(p)], last.at[k, HALF[k], part(p)],
                 sl.at[p, 4 + k], rl.at[p, 4 + k], to)
    for p in range(3):
        total[:, part(p)] += summed(p, coord[p])
    for j in (2, 4):
        for k in range(2):
            half = HALF[1 - k] if j == 2 else HALF[k]
            for p in range(3):
                wait(last.at[k, half, part(p)], rl.at[p, j + k])
                total[half, part(p)] += last[k, half, part(p)].astype(F32)
    y[...] = total[...].astype(BF16)

    for p in range(3):
        for k in range(6):
            if k < 4:
                wait(lines.at[0, HALF[0], part(p)], s1.at[p, k])
            wait(lines.at[0, HALF[0], part(p)], sl.at[p, k])
        wait(tables.at[p, 0:3], st.at[p])
    for g in range(GROUPS):
        wait(out_rows.at[g, :, 0:15], sz.at[g])
        wait(back.at[:, g, 0:15], sc.at[g])


def solution(mesh):
    dma = pltpu.SemaphoreType.DMA

    def body(x, expert, slot, gate, wg, wu, wd, sg, su, sd):
        vmem, anywhere = pl.BlockSpec(memory_space=pltpu.VMEM), pl.BlockSpec(memory_space=pl.ANY)
        out = pl.pallas_call(
            kernel,
            out_shape=jax.ShapeDtypeStruct((T, D), BF16),
            in_specs=[vmem] * 4 + [anywhere] * 6,
            out_specs=vmem,
            scratch_shapes=[
                pltpu.VMEM((4, T, D), BF16),
                pltpu.VMEM((3, 4, 16, 128), F32),
                pltpu.VMEM((3, 4, 16, 128), F32),
                pltpu.VMEM((GROUPS, 4, 16, 8, D), BF16),
                pltpu.VMEM((GROUPS, 4, 4, 4, 8, D), BF16),
                pltpu.VMEM((4, GROUPS, 16, 8, D), BF16),
                pltpu.VMEM((512, D), F32),
                pltpu.VMEM((T, D), F32),
                pltpu.VMEM((2, T // 2, D), BF16),
                pltpu.VMEM((2, T, D), BF16),
                pltpu.VMEM((BUFS, D, TILE), BF16),
                pltpu.VMEM((BUFS, D, TILE), BF16),
                pltpu.VMEM((BUFS, TILE, D), BF16),
                dma((3, 6)), dma((3, 6)), dma((3,)), dma((3,)),
                dma((GROUPS,)), dma((GROUPS,)), dma((GROUPS,)), dma((GROUPS,)),
                dma((3, 6)), dma((3, 6)), dma((BUFS, 3)),
            ],
            compiler_params=pltpu.CompilerParams(has_side_effects=True, collective_id=0, vmem_limit_bytes=67043328),
            name="moe",
        )(x[0, 0], expert[0, 0].T, slot[0, 0].T, gate[0, 0].T, wg, wu, wd, sg, su, sd)
        return out[None, None]

    tokens, experts = P("dp", "ep", None, None), P("ep", None, None)
    return jax.shard_map(body, mesh=mesh, in_specs=(tokens,) * 4 + (experts,) * 3 + (P(None, None),) * 3,
                         out_specs=tokens, check_vma=False)
```

```python
import jax
import jax.numpy as jnp
from jax import lax
from jax.experimental import pallas as pl
from jax.experimental.pallas import tpu as pltpu
from jax.sharding import PartitionSpec as P

F32, BF16 = jnp.float32, jnp.bfloat16
T, D, FF, TOP, SLOTS = 256, 1792, 2048, 8, 20
GROUPS = 5
TILE = 256
STEPS = FF // TILE
BUFS = 3
LANES = ((0, 640), (640, 640), (1280, 512))
OTHERS = ((1, 2), (0, 2), (0, 1))
HALF = (slice(0, T // 2), slice(T // 2, T))
TO_NEXT = ((1, 0), (3, 1), (1, 1), (3, 0))
PASS_ON = 5
MESH = pl.DeviceIdType.MESH
NEAR = tuple((a, b, c) for a in range(4) for b in range(4) for c in range(4) if 0 in (a, b, c) and (a, b, c) != (0, 0, 0))
OFFSETS = tuple((a, b) for a in range(4) for b in range(4) if (a, b) != (0, 0))


def part(p):
    return pl.ds(*LANES[p])


def contract_rows(a, b):
    return lax.dot_general(a, b, (((0,), (0,)), ((), ())), preferred_element_type=F32)


def dot(a, b):
    return jnp.dot(a, b, preferred_element_type=F32)


def kernel(x_hbm, expert, slot, gate, wg, wu, wd, sg, su, sd, y,
           lines, mine, tables, out_rows, z, back, acc, total, hop, last, bg, bu, bd,
           s1, r1, st, rt, sz, rz, sc, rc, sl, rl, wsem, x, xsem):
    me, swap = lax.axis_index("ep"), lax.axis_index("dp") == 1

    def coordinates(d):
        u, v, w = d >> 4, (d >> 2) & 3, d & 3
        return u, jnp.where(swap, w, v), jnp.where(swap, v, w)

    coord = coordinates(me)

    def moved(p, by):
        c = list(coord)
        c[p] = (c[p] + by) % 4
        return c

    def device(c):
        return {"ep": c[0] * 16 + jnp.where(swap, c[2] * 4 + c[1], c[1] * 4 + c[2])}

    def send(src, dst, ss, rs, c):
        pltpu.make_async_remote_copy(src_ref=src, dst_ref=dst, send_sem=ss, recv_sem=rs,
                                     device_id=device(c), device_id_type=MESH).start()

    def wait(like, sem):
        pltpu.make_async_copy(like, like, sem).wait()

    def in_plane(p, c):
        return c[OTHERS[p][0]] * 4 + c[OTHERS[p][1]]

    def rows_of(p, g, c):
        at = [g, *c, slice(None), part(p)]
        at[1 + p] = slice(None)
        return tuple(at)

    def weights(n):
        b = n % BUFS

        @pl.when(n < STEPS)
        def _():
            f = pl.multiple_of(n * TILE, TILE)
            pltpu.make_async_copy(sg.at[:, pl.ds(f, TILE)], bg.at[b], wsem.at[b, 0]).start()
            pltpu.make_async_copy(su.at[:, pl.ds(f, TILE)], bu.at[b], wsem.at[b, 1]).start()
            pltpu.make_async_copy(sd.at[pl.ds(f, TILE), :], bd.at[b], wsem.at[b, 2]).start()

        @pl.when((n >= STEPS) & (n < 7 * STEPS))
        def _():
            e = (n - STEPS) // (3 * STEPS)
            f = pl.multiple_of((n % STEPS) * TILE, TILE)
            pltpu.make_async_copy(wg.at[e, :, pl.ds(f, TILE)], bg.at[b], wsem.at[b, 0]).start()
            pltpu.make_async_copy(wu.at[e, :, pl.ds(f, TILE)], bu.at[b], wsem.at[b, 1]).start()
            pltpu.make_async_copy(wd.at[e, pl.ds(f, TILE), :], bd.at[b], wsem.at[b, 2]).start()

    def ready(n):
        b = n % BUFS
        wait(bg.at[b], wsem.at[b, 0])
        wait(bu.at[b], wsem.at[b, 1])
        wait(bd.at[b], wsem.at[b, 2])
        return b

    pltpu.make_async_copy(x_hbm, x, xsem).start()

    entered = pltpu.get_barrier_semaphore()
    for by in NEAR:
        to = [(v + d) % 4 for v, d in zip(coord, by)]
        pl.semaphore_signal(entered, inc=1, device_id=device(to), device_id_type=MESH)
    weights(0)
    weights(1)

    ex, sl_ = expert[...], slot[...]
    c, at = coordinates(ex >> 1), (ex & 1) * SLOTS + sl_
    valid = sl_ < SLOTS
    g8, j8 = at >> 3, at & 7
    gates = gate[...].astype(BF16).astype(F32)
    along = lax.broadcasted_iota(jnp.int32, (128, T), 1).astype(F32) + 1.0
    down = lax.broadcasted_iota(jnp.int32, (128, T), 0)
    for p in range(3):
        row = jnp.where(valid, c[p] * 8 + g8, -1)
        col = (c[OTHERS[p][0]] * 4 + c[OTHERS[p][1]]) * 8 + j8
        table = jnp.zeros((32, 256), F32)
        for k in range(TOP):
            left = (down[:32] == row[k:k + 1, :]).astype(BF16)
            here = down == col[k:k + 1, :]
            right = jnp.concatenate([jnp.where(here, along, 0.0), jnp.where(here, gates[k:k + 1, :], 0.0)], axis=0)
            table += lax.dot_general(left, right.astype(BF16), (((1,), (1,)), ((), ())), preferred_element_type=F32)
        for i in range(4):
            mine[p, i, 0:8, :] = table[8 * i:8 * i + 8, :128]
            mine[p, i, 8:16, :] = table[8 * i:8 * i + 8, 128:]
        tables[p, coord[p]] = mine[p, coord[p]]
    number = lax.broadcasted_iota(jnp.int32, (T, 128), 0).astype(F32) + 1.0
    wait(x, xsem)
    pl.semaphore_wait(entered, len(NEAR))

    for by in (2, 1, 3):
        for p in range(3):
            to = moved(p, by)
            send(mine.at[p, to[p]], tables.at[p, coord[p]], st.at[p], rt.at[p], to)
    for first, half in ((1, 0), (3, 1), (1, 1), (3, 0)):
        for p in range(3):
            k = TO_NEXT.index((first, half))
            send(x.at[HALF[half], part(p)], lines.at[coord[p], HALF[half], part(p)],
                 s1.at[p, k], r1.at[p, k], moved(p, first))
    for p in range(3):
        lines[coord[p], :, part(p)] = x[:, part(p)]

    total[...] = jnp.zeros_like(total)

    def pass_on():
        for k, (first, half) in enumerate(TO_NEXT[:2]):
            for p in range(3):
                i = moved(p, 4 - first)[p]
                arrived = lines.at[i, HALF[half], part(p)]
                wait(arrived, r1.at[p, k])
                send(arrived, arrived, s1.at[p, 4 + k], r1.at[p, 4 + k], moved(p, first))

    def shared(n, _):
        @pl.when(n == PASS_ON)
        def _():
            pass_on()

        weights(n + 2)
        b = ready(n)
        h = jax.nn.silu(dot(x[...], bg[b])) * dot(x[...], bu[b])
        total[...] += dot(h.astype(BF16), bd[b])
        return 0

    lax.fori_loop(0, STEPS, shared, 0)
    def plane(p):
        for a, b in OFFSETS:
            to = list(coord)
            to[OTHERS[p][0]] = (to[OTHERS[p][0]] + a) % 4
            to[OTHERS[p][1]] = (to[OTHERS[p][1]] + b) % 4
            yield to

    def pick(p, g, i):
        chosen = (number == tables[p, i, pl.ds(g, 1), :]).astype(BF16)
        rows = contract_rows(chosen, lines[i, :, part(p)]).astype(BF16)
        out_rows[g, i, :, :, part(p)] = rows.reshape(16, 8, LANES[p][1])

    def keep(g):
        for p in range(3):
            z[rows_of(p, g, coord)] = out_rows[g, :, in_plane(p, coord), :, part(p)]

    def dispatch(g):
        for p in range(3):
            for i in range(4):
                pick(p, g, i)
            for to in plane(p):
                send(out_rows.at[g, :, in_plane(p, to), :, part(p)], z.at[rows_of(p, g, coord)],
                     sz.at[g], rz.at[g], to)
        keep(g)

    for by, arrivals in ((0, ()), (1, (3,)), (3, (2,)), (2, (4, 5))):
        for p in range(3):
            source = moved(p, by)
            if by == 1:
                wait(tables.at[p, 0:3], rt.at[p])
            for k in arrivals:
                wait(lines.at[0, HALF[0], part(p)], r1.at[p, k])
            pick(p, 0, source[p])
            for to in plane(p):
                send(out_rows.at[0, source[p], in_plane(p, to), :, part(p)], z.at[(0, *source, slice(None), part(p))],
                     sz.at[0], rz.at[0], to)
    keep(0)

    def give_back(g):
        for a, b in OFFSETS:
            for p in range(3):
                to = list(coord)
                to[OTHERS[p][0]] = (to[OTHERS[p][0]] + a) % 4
                to[OTHERS[p][1]] = (to[OTHERS[p][1]] + b) % 4
                send(z.at[rows_of(p, g, to)], back.at[:, g, in_plane(p, coord), :, part(p)],
                     sc.at[g], rc.at[g], to)
        for p in range(3):
            back[:, g, in_plane(p, coord), :, part(p)] = z[rows_of(p, g, coord)]

    def experts(i):
        e = i // 3
        g = i - e

        @pl.when(i != 3)
        def _():
            wait(out_rows.at[g, :, 0:15], rz.at[g])
            acc[...] = jnp.zeros_like(acc)

        at = g * 8 + (lax.broadcasted_iota(jnp.int32, (512, TILE), 0) & 7)
        own = (at >= SLOTS) == (e == 1)

        def step(f, _):
            n = STEPS + i * STEPS + f
            weights(n + 2)
            b = ready(n)
            rows = z[g].reshape(512, D)
            h = jax.nn.silu(dot(rows, bg[b])) * dot(rows, bu[b])
            acc[...] += dot(jnp.where(own, h, 0.0).astype(BF16), bd[b])
            return 0

        lax.fori_loop(0, STEPS, step, 0)

        @pl.when(i != 2)
        def _():
            z[g] = acc[...].astype(BF16).reshape(4, 4, 4, 8, D)
            give_back(g)

    def each(f):
        def run(i, _):
            f(i)
            return 0

        return run

    lax.fori_loop(1, GROUPS, each(dispatch), 0)
    lax.fori_loop(0, GROUPS + 1, each(experts), 0)

    for g in range(GROUPS):
        wait(back.at[:, g, 0:15], rc.at[g])
    def summed(p, i):
        mix = jnp.concatenate(
            [jnp.where(number == tables[p, i, g:g + 1, :], tables[p, i, 8 + g:9 + g, :], 0.0).astype(BF16)
             for g in range(GROUPS)], axis=1)
        return dot(mix, back[i, :, :, :, part(p)].reshape(GROUPS * 128, LANES[p][1]))

    for p in range(3):
        for k in range(2):
            wait(lines.at[0, HALF[0], part(p)], s1.at[p, 4 + k])
    for p in range(3):
        i = moved(p, 2)[p]
        lines[i, :, part(p)] = summed(p, i).astype(BF16)
        for k, by in enumerate((3, 1)):
            send(lines.at[i, HALF[k], part(p)], hop.at[k, :, part(p)], sl.at[p, k], rl.at[p, k], moved(p, by))
    for k, by in enumerate((3, 1)):
        for p in range(3):
            to = moved(p, by)
            own = summed(p, to[p])
            lines[to[p], HALF[1 - k], part(p)] = own[HALF[1 - k]].astype(BF16)
            send(lines.at[to[p], HALF[1 - k], part(p)], last.at[k, HALF[1 - k], part(p)],
                 sl.at[p, 2 + k], rl.at[p, 2 + k], to)
            acc[HALF[k], part(p)] = own[HALF[k]]
    for k, by in enumerate((3, 1)):
        for p in range(3):
            to = moved(p, by)
            wait(hop.at[k, :, part(p)], rl.at[p, k])
            both = acc[HALF[k], part(p)] + hop[k, :, part(p)].astype(F32)
            lines[to[p], HALF[k], part(p)] = both.astype(BF16)
            send(lines.at[to[p], HALF[k], part(p)], last.at[k, HALF[k], part(p)],
                 sl.at[p, 4 + k], rl.at[p, 4 + k], to)
    for p in range(3):
        total[:, part(p)] += summed(p, coord[p])
    for j in (2, 4):
        for k in range(2):
            half = HALF[1 - k] if j == 2 else HALF[k]
            for p in range(3):
                wait(last.at[k, half, part(p)], rl.at[p, j + k])
                total[half, part(p)] += last[k, half, part(p)].astype(F32)
    y[...] = total[...].astype(BF16)

    for p in range(3):
        for k in range(6):
            if k < 4:
                wait(lines.at[0, HALF[0], part(p)], s1.at[p, k])
            wait(lines.at[0, HALF[0], part(p)], sl.at[p, k])
        wait(tables.at[p, 0:3], st.at[p])
    for g in range(GROUPS):
        wait(out_rows.at[g, :, 0:15], sz.at[g])
        wait(back.at[:, g, 0:15], sc.at[g])


def solution(mesh):
    dma = pltpu.SemaphoreType.DMA

    def body(x, expert, slot, gate, wg, wu, wd, sg, su, sd):
        vmem, anywhere = pl.BlockSpec(memory_space=pltpu.VMEM), pl.BlockSpec(memory_space=pl.ANY)
        out = pl.pallas_call(
            kernel,
            out_shape=jax.ShapeDtypeStruct((T, D), BF16),
            in_specs=[anywhere] + [vmem] * 3 + [anywhere] * 6,
            out_specs=vmem,
            scratch_shapes=[
                pltpu.VMEM((4, T, D), BF16),
                pltpu.VMEM((3, 4, 16, 128), F32),
                pltpu.VMEM((3, 4, 16, 128), F32),
                pltpu.VMEM((GROUPS, 4, 16, 8, D), BF16),
                pltpu.VMEM((GROUPS, 4, 4, 4, 8, D), BF16),
                pltpu.VMEM((4, GROUPS, 16, 8, D), BF16),
                pltpu.VMEM((512, D), F32),
                pltpu.VMEM((T, D), F32),
                pltpu.VMEM((2, T // 2, D), BF16),
                pltpu.VMEM((2, T, D), BF16),
                pltpu.VMEM((BUFS, D, TILE), BF16),
                pltpu.VMEM((BUFS, D, TILE), BF16),
                pltpu.VMEM((BUFS, TILE, D), BF16),
                dma((3, 6)), dma((3, 6)), dma((3,)), dma((3,)),
                dma((GROUPS,)), dma((GROUPS,)), dma((GROUPS,)), dma((GROUPS,)),
                dma((3, 6)), dma((3, 6)), dma((BUFS, 3)),
                pltpu.VMEM((T, D), BF16), dma(()),
            ],
            compiler_params=pltpu.CompilerParams(has_side_effects=True, collective_id=0, vmem_limit_bytes=67043328),
            name="moe",
        )(x[0, 0], expert[0, 0].T, slot[0, 0].T, gate[0, 0].T, wg, wu, wd, sg, su, sd)
        return out[None, None]

    tokens, experts = P("dp", "ep", None, None), P("ep", None, None)
    return jax.shard_map(body, mesh=mesh, in_specs=(tokens,) * 4 + (experts,) * 3 + (P(None, None),) * 3,
                         out_specs=tokens, check_vma=False)
```

```python
import jax
import jax.numpy as jnp
from jax import lax
from jax.experimental import pallas as pl
from jax.experimental.pallas import tpu as pltpu
from jax.sharding import PartitionSpec as P

F32, BF16 = jnp.float32, jnp.bfloat16
T, D, FF, TOP, SLOTS = 256, 1792, 2048, 8, 20
GROUPS = 5
TILE = 256
STEPS = FF // TILE
BUFS = 3
LANES = ((0, 640), (640, 640), (1280, 512))
OTHERS = ((1, 2), (0, 2), (0, 1))
HALF = (slice(0, T // 2), slice(T // 2, T))
TO_NEXT = ((1, 0), (3, 1), (1, 1), (3, 0))
PASS_ON = 5
MESH = pl.DeviceIdType.MESH
NEAR = tuple((a, b, c) for a in range(4) for b in range(4) for c in range(4) if 0 in (a, b, c) and (a, b, c) != (0, 0, 0))
OFFSETS = tuple((a, b) for a in range(4) for b in range(4) if (a, b) != (0, 0))


def part(p):
    return pl.ds(*LANES[p])


def contract_rows(a, b):
    return lax.dot_general(a, b, (((0,), (0,)), ((), ())), preferred_element_type=F32)


def dot(a, b):
    return jnp.dot(a, b, preferred_element_type=F32)


def kernel(x_hbm, e_hbm, s_hbm, g_hbm, wg, wu, wd, sg, su, sd, y_hbm,
           lines, mine, tables, out_rows, z, back, acc, total, hop, last, bg, bu, bd,
           s1, r1, st, rt, sz, rz, sc, rc, sl, rl, wsem, x, xsem, expert, slot, gate, esem, y, ysem):
    me, swap = lax.axis_index("ep"), lax.axis_index("dp") == 1

    def coordinates(d):
        u, v, w = d >> 4, (d >> 2) & 3, d & 3
        return u, jnp.where(swap, w, v), jnp.where(swap, v, w)

    coord = coordinates(me)

    def moved(p, by):
        c = list(coord)
        c[p] = (c[p] + by) % 4
        return c

    def device(c):
        return {"ep": c[0] * 16 + jnp.where(swap, c[2] * 4 + c[1], c[1] * 4 + c[2])}

    def send(src, dst, ss, rs, c):
        pltpu.make_async_remote_copy(src_ref=src, dst_ref=dst, send_sem=ss, recv_sem=rs,
                                     device_id=device(c), device_id_type=MESH).start()

    def wait(like, sem):
        pltpu.make_async_copy(like, like, sem).wait()

    def in_plane(p, c):
        return c[OTHERS[p][0]] * 4 + c[OTHERS[p][1]]

    def rows_of(p, g, c):
        at = [g, *c, slice(None), part(p)]
        at[1 + p] = slice(None)
        return tuple(at)

    def weights(n):
        b = n % BUFS

        @pl.when(n < STEPS)
        def _():
            f = pl.multiple_of(n * TILE, TILE)
            pltpu.make_async_copy(sg.at[:, pl.ds(f, TILE)], bg.at[b], wsem.at[b, 0]).start()
            pltpu.make_async_copy(su.at[:, pl.ds(f, TILE)], bu.at[b], wsem.at[b, 1]).start()
            pltpu.make_async_copy(sd.at[pl.ds(f, TILE), :], bd.at[b], wsem.at[b, 2]).start()

        @pl.when((n >= STEPS) & (n < 7 * STEPS))
        def _():
            e = (n - STEPS) // (3 * STEPS)
            f = pl.multiple_of((n % STEPS) * TILE, TILE)
            pltpu.make_async_copy(wg.at[e, :, pl.ds(f, TILE)], bg.at[b], wsem.at[b, 0]).start()
            pltpu.make_async_copy(wu.at[e, :, pl.ds(f, TILE)], bu.at[b], wsem.at[b, 1]).start()
            pltpu.make_async_copy(wd.at[e, pl.ds(f, TILE), :], bd.at[b], wsem.at[b, 2]).start()

    def ready(n):
        b = n % BUFS
        wait(bg.at[b], wsem.at[b, 0])
        wait(bu.at[b], wsem.at[b, 1])
        wait(bd.at[b], wsem.at[b, 2])
        return b

    entered = pltpu.get_barrier_semaphore()
    for by in NEAR:
        to = [(v + d) % 4 for v, d in zip(coord, by)]
        pl.semaphore_signal(entered, inc=1, device_id=device(to), device_id_type=MESH)
    routing = tuple(pltpu.make_async_copy(a, b, esem.at[n])
                    for n, (a, b) in enumerate(((e_hbm, expert), (s_hbm, slot), (g_hbm, gate))))
    for copy in routing:
        copy.start()
    pltpu.make_async_copy(x_hbm, x, xsem).start()
    weights(0)
    weights(1)

    for copy in routing:
        copy.wait()
    ex, sl_ = expert[...], slot[...]
    c, at = coordinates(ex >> 1), (ex & 1) * SLOTS + sl_
    valid = sl_ < SLOTS
    g8, j8 = at >> 3, at & 7
    gates = gate[...].astype(BF16).astype(F32)
    along = lax.broadcasted_iota(jnp.int32, (128, T), 1).astype(F32) + 1.0
    down = lax.broadcasted_iota(jnp.int32, (128, T), 0)
    for p in range(3):
        row = jnp.where(valid, c[p] * 8 + g8, -1)
        col = (c[OTHERS[p][0]] * 4 + c[OTHERS[p][1]]) * 8 + j8
        table = jnp.zeros((32, 256), F32)
        for k in range(TOP):
            left = (down[:32] == row[k:k + 1, :]).astype(BF16)
            here = down == col[k:k + 1, :]
            right = jnp.concatenate([jnp.where(here, along, 0.0), jnp.where(here, gates[k:k + 1, :], 0.0)], axis=0)
            table += lax.dot_general(left, right.astype(BF16), (((1,), (1,)), ((), ())), preferred_element_type=F32)
        for i in range(4):
            mine[p, i, 0:8, :] = table[8 * i:8 * i + 8, :128]
            mine[p, i, 8:16, :] = table[8 * i:8 * i + 8, 128:]
        tables[p, coord[p]] = mine[p, coord[p]]
    number = lax.broadcasted_iota(jnp.int32, (T, 128), 0).astype(F32) + 1.0
    wait(x, xsem)
    pl.semaphore_wait(entered, len(NEAR))

    for by in (2, 1, 3):
        for p in range(3):
            to = moved(p, by)
            send(mine.at[p, to[p]], tables.at[p, coord[p]], st.at[p], rt.at[p], to)
    for first, half in ((1, 0), (3, 1), (1, 1), (3, 0)):
        for p in range(3):
            k = TO_NEXT.index((first, half))
            send(x.at[HALF[half], part(p)], lines.at[coord[p], HALF[half], part(p)],
                 s1.at[p, k], r1.at[p, k], moved(p, first))
    for p in range(3):
        lines[coord[p], :, part(p)] = x[:, part(p)]

    total[...] = jnp.zeros_like(total)

    def pass_on():
        for k, (first, half) in enumerate(TO_NEXT[:2]):
            for p in range(3):
                i = moved(p, 4 - first)[p]
                arrived = lines.at[i, HALF[half], part(p)]
                wait(arrived, r1.at[p, k])
                send(arrived, arrived, s1.at[p, 4 + k], r1.at[p, 4 + k], moved(p, first))

    def shared(n, _):
        @pl.when(n == PASS_ON)
        def _():
            pass_on()

        weights(n + 2)
        b = ready(n)
        h = jax.nn.silu(dot(x[...], bg[b])) * dot(x[...], bu[b])
        total[...] += dot(h.astype(BF16), bd[b])
        return 0

    lax.fori_loop(0, STEPS, shared, 0)
    def plane(p):
        for a, b in OFFSETS:
            to = list(coord)
            to[OTHERS[p][0]] = (to[OTHERS[p][0]] + a) % 4
            to[OTHERS[p][1]] = (to[OTHERS[p][1]] + b) % 4
            yield to

    def pick(p, g, i):
        chosen = (number == tables[p, i, pl.ds(g, 1), :]).astype(BF16)
        rows = contract_rows(chosen, lines[i, :, part(p)]).astype(BF16)
        out_rows[g, i, :, :, part(p)] = rows.reshape(16, 8, LANES[p][1])

    def keep(g):
        for p in range(3):
            z[rows_of(p, g, coord)] = out_rows[g, :, in_plane(p, coord), :, part(p)]

    def dispatch(g):
        for p in range(3):
            for i in range(4):
                pick(p, g, i)
            for to in plane(p):
                send(out_rows.at[g, :, in_plane(p, to), :, part(p)], z.at[rows_of(p, g, coord)],
                     sz.at[g], rz.at[g], to)
        keep(g)

    for by, arrivals in ((0, ()), (1, (3,)), (3, (2,)), (2, (4, 5))):
        for p in range(3):
            source = moved(p, by)
            if by == 1:
                wait(tables.at[p, 0:3], rt.at[p])
            for k in arrivals:
                wait(lines.at[0, HALF[0], part(p)], r1.at[p, k])
            pick(p, 0, source[p])
            for to in plane(p):
                send(out_rows.at[0, source[p], in_plane(p, to), :, part(p)], z.at[(0, *source, slice(None), part(p))],
                     sz.at[0], rz.at[0], to)
    keep(0)

    def give_back(g):
        for a, b in OFFSETS:
            for p in range(3):
                to = list(coord)
                to[OTHERS[p][0]] = (to[OTHERS[p][0]] + a) % 4
                to[OTHERS[p][1]] = (to[OTHERS[p][1]] + b) % 4
                send(z.at[rows_of(p, g, to)], back.at[:, g, in_plane(p, coord), :, part(p)],
                     sc.at[g], rc.at[g], to)
        for p in range(3):
            back[:, g, in_plane(p, coord), :, part(p)] = z[rows_of(p, g, coord)]

    def experts(i):
        e = i // 3
        g = i - e

        @pl.when(i != 3)
        def _():
            wait(out_rows.at[g, :, 0:15], rz.at[g])
            acc[...] = jnp.zeros_like(acc)

        at = g * 8 + (lax.broadcasted_iota(jnp.int32, (512, TILE), 0) & 7)
        own = (at >= SLOTS) == (e == 1)

        def step(f, _):
            n = STEPS + i * STEPS + f
            weights(n + 2)
            b = ready(n)
            rows = z[g].reshape(512, D)
            h = jax.nn.silu(dot(rows, bg[b])) * dot(rows, bu[b])
            acc[...] += dot(jnp.where(own, h, 0.0).astype(BF16), bd[b])
            return 0

        lax.fori_loop(0, STEPS, step, 0)

        @pl.when(i != 2)
        def _():
            z[g] = acc[...].astype(BF16).reshape(4, 4, 4, 8, D)
            give_back(g)

    def each(f):
        def run(i, _):
            f(i)
            return 0

        return run

    lax.fori_loop(1, GROUPS, each(dispatch), 0)
    lax.fori_loop(0, GROUPS + 1, each(experts), 0)

    for g in range(GROUPS):
        wait(back.at[:, g, 0:15], rc.at[g])
    def summed(p, i):
        mix = jnp.concatenate(
            [jnp.where(number == tables[p, i, g:g + 1, :], tables[p, i, 8 + g:9 + g, :], 0.0).astype(BF16)
             for g in range(GROUPS)], axis=1)
        return dot(mix, back[i, :, :, :, part(p)].reshape(GROUPS * 128, LANES[p][1]))

    for p in range(3):
        for k in range(2):
            wait(lines.at[0, HALF[0], part(p)], s1.at[p, 4 + k])
    for p in range(3):
        i = moved(p, 2)[p]
        lines[i, :, part(p)] = summed(p, i).astype(BF16)
        for k, by in enumerate((3, 1)):
            send(lines.at[i, HALF[k], part(p)], hop.at[k, :, part(p)], sl.at[p, k], rl.at[p, k], moved(p, by))
    for k, by in enumerate((3, 1)):
        for p in range(3):
            to = moved(p, by)
            own = summed(p, to[p])
            lines[to[p], HALF[1 - k], part(p)] = own[HALF[1 - k]].astype(BF16)
            send(lines.at[to[p], HALF[1 - k], part(p)], last.at[k, HALF[1 - k], part(p)],
                 sl.at[p, 2 + k], rl.at[p, 2 + k], to)
            acc[HALF[k], part(p)] = own[HALF[k]]
    for k, by in enumerate((3, 1)):
        for p in range(3):
            to = moved(p, by)
            wait(hop.at[k, :, part(p)], rl.at[p, k])
            both = acc[HALF[k], part(p)] + hop[k, :, part(p)].astype(F32)
            lines[to[p], HALF[k], part(p)] = both.astype(BF16)
            send(lines.at[to[p], HALF[k], part(p)], last.at[k, HALF[k], part(p)],
                 sl.at[p, 4 + k], rl.at[p, 4 + k], to)
    for p in range(3):
        total[:, part(p)] += summed(p, coord[p])
    for j in (2, 4):
        for k in range(2):
            half = HALF[1 - k] if j == 2 else HALF[k]
            for p in range(3):
                wait(last.at[k, half, part(p)], rl.at[p, j + k])
                both = total[half, part(p)] + last[k, half, part(p)].astype(F32)
                if j == 2:
                    total[half, part(p)] = both
                else:
                    y[half, part(p)] = both.astype(BF16)
                    pltpu.make_async_copy(y.at[half, part(p)], y_hbm.at[half, part(p)], ysem.at[k, p]).start()
    for k in range(2):
        for p in range(3):
            wait(y.at[HALF[k], part(p)], ysem.at[k, p])

    for p in range(3):
        for k in range(6):
            if k < 4:
                wait(lines.at[0, HALF[0], part(p)], s1.at[p, k])
            wait(lines.at[0, HALF[0], part(p)], sl.at[p, k])
        wait(tables.at[p, 0:3], st.at[p])
    for g in range(GROUPS):
        wait(out_rows.at[g, :, 0:15], sz.at[g])
        wait(back.at[:, g, 0:15], sc.at[g])


def solution(mesh):
    dma = pltpu.SemaphoreType.DMA

    def body(x, expert, slot, gate, wg, wu, wd, sg, su, sd):
        anywhere = pl.BlockSpec(memory_space=pl.ANY)
        out = pl.pallas_call(
            kernel,
            out_shape=jax.ShapeDtypeStruct((T, D), BF16),
            in_specs=[anywhere] * 10,
            out_specs=anywhere,
            scratch_shapes=[
                pltpu.VMEM((4, T, D), BF16),
                pltpu.VMEM((3, 4, 16, 128), F32),
                pltpu.VMEM((3, 4, 16, 128), F32),
                pltpu.VMEM((GROUPS, 4, 16, 8, D), BF16),
                pltpu.VMEM((GROUPS, 4, 4, 4, 8, D), BF16),
                pltpu.VMEM((4, GROUPS, 16, 8, D), BF16),
                pltpu.VMEM((512, D), F32),
                pltpu.VMEM((T, D), F32),
                pltpu.VMEM((2, T // 2, D), BF16),
                pltpu.VMEM((2, T, D), BF16),
                pltpu.VMEM((BUFS, D, TILE), BF16),
                pltpu.VMEM((BUFS, D, TILE), BF16),
                pltpu.VMEM((BUFS, TILE, D), BF16),
                dma((3, 6)), dma((3, 6)), dma((3,)), dma((3,)),
                dma((GROUPS,)), dma((GROUPS,)), dma((GROUPS,)), dma((GROUPS,)),
                dma((3, 6)), dma((3, 6)), dma((BUFS, 3)),
                pltpu.VMEM((T, D), BF16), dma(()),
                pltpu.VMEM((TOP, T), jnp.int32), pltpu.VMEM((TOP, T), jnp.int32), pltpu.VMEM((TOP, T), F32), dma((3,)),
                pltpu.VMEM((T, D), BF16), dma((2, 3)),
            ],
            compiler_params=pltpu.CompilerParams(has_side_effects=True, collective_id=0, vmem_limit_bytes=67043328),
            name="moe",
        )(x[0, 0], expert[0, 0].T, slot[0, 0].T, gate[0, 0].T, wg, wu, wd, sg, su, sd)
        return out[None, None]

    tokens, experts = P("dp", "ep", None, None), P("ep", None, None)
    return jax.shard_map(body, mesh=mesh, in_specs=(tokens,) * 4 + (experts,) * 3 + (P(None, None),) * 3,
                         out_specs=tokens, check_vma=False)
```

```python
import jax
import jax.numpy as jnp
from jax import lax
from jax.experimental import pallas as pl
from jax.experimental.pallas import tpu as pltpu
from jax.sharding import PartitionSpec as P

F32, BF16 = jnp.float32, jnp.bfloat16
T, D, FF, TOP, SLOTS = 256, 1792, 2048, 8, 20
GROUPS = 5
TILE = 256
STEPS = FF // TILE
BUFS = 3
LANES = ((0, 640), (640, 640), (1280, 512))
OTHERS = ((1, 2), (0, 2), (0, 1))
HALF = (slice(0, T // 2), slice(T // 2, T))
TO_NEXT = ((1, 0), (3, 1), (1, 1), (3, 0))
PASS_ON = 5
MESH = pl.DeviceIdType.MESH
OFFSETS = tuple((a, b) for a in range(4) for b in range(4) if (a, b) != (0, 0))


def part(p):
    return pl.ds(*LANES[p])


def contract_rows(a, b):
    return lax.dot_general(a, b, (((0,), (0,)), ((), ())), preferred_element_type=F32)


def dot(a, b):
    return jnp.dot(a, b, preferred_element_type=F32)


def kernel(x_hbm, e_hbm, s_hbm, g_hbm, wg, wu, wd, sg, su, sd, y_hbm,
           lines, mine, tables, out_rows, z, back, acc, total, hop, last, bg, bu, bd,
           s1, r1, st, rt, sz, rz, sc, rc, sl, rl, wsem, x, xsem, expert, slot, gate, esem, y, ysem, met):
    me, swap = lax.axis_index("ep"), lax.axis_index("dp") == 1

    def coordinates(d):
        u, v, w = d >> 4, (d >> 2) & 3, d & 3
        return u, jnp.where(swap, w, v), jnp.where(swap, v, w)

    coord = coordinates(me)

    def moved(p, by):
        c = list(coord)
        c[p] = (c[p] + by) % 4
        return c

    def device(c):
        return {"ep": c[0] * 16 + jnp.where(swap, c[2] * 4 + c[1], c[1] * 4 + c[2])}

    def send(src, dst, ss, rs, c):
        pltpu.make_async_remote_copy(src_ref=src, dst_ref=dst, send_sem=ss, recv_sem=rs,
                                     device_id=device(c), device_id_type=MESH).start()

    def wait(like, sem):
        pltpu.make_async_copy(like, like, sem).wait()

    def in_plane(p, c):
        return c[OTHERS[p][0]] * 4 + c[OTHERS[p][1]]

    def rows_of(p, g, c):
        at = [g, *c, slice(None), part(p)]
        at[1 + p] = slice(None)
        return tuple(at)

    def weights(n):
        b = n % BUFS

        @pl.when(n < STEPS)
        def _():
            f = pl.multiple_of(n * TILE, TILE)
            pltpu.make_async_copy(sg.at[:, pl.ds(f, TILE)], bg.at[b], wsem.at[b, 0]).start()
            pltpu.make_async_copy(su.at[:, pl.ds(f, TILE)], bu.at[b], wsem.at[b, 1]).start()
            pltpu.make_async_copy(sd.at[pl.ds(f, TILE), :], bd.at[b], wsem.at[b, 2]).start()

        @pl.when((n >= STEPS) & (n < 7 * STEPS))
        def _():
            e = (n - STEPS) // (3 * STEPS)
            f = pl.multiple_of((n % STEPS) * TILE, TILE)
            pltpu.make_async_copy(wg.at[e, :, pl.ds(f, TILE)], bg.at[b], wsem.at[b, 0]).start()
            pltpu.make_async_copy(wu.at[e, :, pl.ds(f, TILE)], bu.at[b], wsem.at[b, 1]).start()
            pltpu.make_async_copy(wd.at[e, pl.ds(f, TILE), :], bd.at[b], wsem.at[b, 2]).start()

    def ready(n):
        b = n % BUFS
        wait(bg.at[b], wsem.at[b, 0])
        wait(bu.at[b], wsem.at[b, 1])
        wait(bd.at[b], wsem.at[b, 2])
        return b

    entered = pltpu.get_barrier_semaphore()
    peers = [moved(p, by) for p in range(3) for by in (1, 2, 3)]
    for to in peers:
        pl.semaphore_signal(entered, inc=1, device_id=device(to), device_id_type=MESH)
    routing = tuple(pltpu.make_async_copy(a, b, esem.at[n])
                    for n, (a, b) in enumerate(((e_hbm, expert), (s_hbm, slot), (g_hbm, gate))))
    for copy in routing:
        copy.start()
    pltpu.make_async_copy(x_hbm, x, xsem).start()
    weights(0)
    weights(1)

    for copy in routing:
        copy.wait()
    ex, sl_ = expert[...], slot[...]
    c, at = coordinates(ex >> 1), (ex & 1) * SLOTS + sl_
    valid = sl_ < SLOTS
    g8, j8 = at >> 3, at & 7
    gates = gate[...].astype(BF16).astype(F32)
    along = lax.broadcasted_iota(jnp.int32, (128, T), 1).astype(F32) + 1.0
    down = lax.broadcasted_iota(jnp.int32, (128, T), 0)
    for p in range(3):
        row = jnp.where(valid, c[p] * 8 + g8, -1)
        col = (c[OTHERS[p][0]] * 4 + c[OTHERS[p][1]]) * 8 + j8
        table = jnp.zeros((32, 256), F32)
        for k in range(TOP):
            left = (down[:32] == row[k:k + 1, :]).astype(BF16)
            here = down == col[k:k + 1, :]
            right = jnp.concatenate([jnp.where(here, along, 0.0), jnp.where(here, gates[k:k + 1, :], 0.0)], axis=0)
            table += lax.dot_general(left, right.astype(BF16), (((1,), (1,)), ((), ())), preferred_element_type=F32)
        for i in range(4):
            mine[p, i, 0:8, :] = table[8 * i:8 * i + 8, :128]
            mine[p, i, 8:16, :] = table[8 * i:8 * i + 8, 128:]
        tables[p, coord[p]] = mine[p, coord[p]]
    number = lax.broadcasted_iota(jnp.int32, (T, 128), 0).astype(F32) + 1.0
    wait(x, xsem)
    pl.semaphore_wait(entered, len(peers))
    for to in peers:
        pl.semaphore_signal(met, inc=1, device_id=device(to), device_id_type=MESH)

    for by in (2, 1, 3):
        for p in range(3):
            to = moved(p, by)
            send(mine.at[p, to[p]], tables.at[p, coord[p]], st.at[p], rt.at[p], to)
    for first, half in ((1, 0), (3, 1), (1, 1), (3, 0)):
        for p in range(3):
            k = TO_NEXT.index((first, half))
            send(x.at[HALF[half], part(p)], lines.at[coord[p], HALF[half], part(p)],
                 s1.at[p, k], r1.at[p, k], moved(p, first))
    for p in range(3):
        lines[coord[p], :, part(p)] = x[:, part(p)]

    total[...] = jnp.zeros_like(total)

    def pass_on():
        for k, (first, half) in enumerate(TO_NEXT[:2]):
            for p in range(3):
                i = moved(p, 4 - first)[p]
                arrived = lines.at[i, HALF[half], part(p)]
                wait(arrived, r1.at[p, k])
                send(arrived, arrived, s1.at[p, 4 + k], r1.at[p, 4 + k], moved(p, first))

    def shared(n, _):
        @pl.when(n == PASS_ON)
        def _():
            pass_on()

        weights(n + 2)
        b = ready(n)
        h = jax.nn.silu(dot(x[...], bg[b])) * dot(x[...], bu[b])
        total[...] += dot(h.astype(BF16), bd[b])
        return 0

    lax.fori_loop(0, STEPS, shared, 0)
    def plane(p):
        for a, b in OFFSETS:
            to = list(coord)
            to[OTHERS[p][0]] = (to[OTHERS[p][0]] + a) % 4
            to[OTHERS[p][1]] = (to[OTHERS[p][1]] + b) % 4
            yield to

    def pick(p, g, i):
        chosen = (number == tables[p, i, pl.ds(g, 1), :]).astype(BF16)
        rows = contract_rows(chosen, lines[i, :, part(p)]).astype(BF16)
        out_rows[g, i, :, :, part(p)] = rows.reshape(16, 8, LANES[p][1])

    def keep(g):
        for p in range(3):
            z[rows_of(p, g, coord)] = out_rows[g, :, in_plane(p, coord), :, part(p)]

    def dispatch(g):
        for p in range(3):
            for i in range(4):
                pick(p, g, i)
            for to in plane(p):
                send(out_rows.at[g, :, in_plane(p, to), :, part(p)], z.at[rows_of(p, g, coord)],
                     sz.at[g], rz.at[g], to)
        keep(g)

    pl.semaphore_wait(met, len(peers))

    for by, arrivals in ((0, ()), (1, (3,)), (3, (2,)), (2, (4, 5))):
        for p in range(3):
            source = moved(p, by)
            if by == 1:
                wait(tables.at[p, 0:3], rt.at[p])
            for k in arrivals:
                wait(lines.at[0, HALF[0], part(p)], r1.at[p, k])
            pick(p, 0, source[p])
            for to in plane(p):
                send(out_rows.at[0, source[p], in_plane(p, to), :, part(p)], z.at[(0, *source, slice(None), part(p))],
                     sz.at[0], rz.at[0], to)
    keep(0)

    def give_back(g):
        for a, b in OFFSETS:
            for p in range(3):
                to = list(coord)
                to[OTHERS[p][0]] = (to[OTHERS[p][0]] + a) % 4
                to[OTHERS[p][1]] = (to[OTHERS[p][1]] + b) % 4
                send(z.at[rows_of(p, g, to)], back.at[:, g, in_plane(p, coord), :, part(p)],
                     sc.at[g], rc.at[g], to)
        for p in range(3):
            back[:, g, in_plane(p, coord), :, part(p)] = z[rows_of(p, g, coord)]

    def experts(i):
        e = i // 3
        g = i - e

        @pl.when(i != 3)
        def _():
            wait(out_rows.at[g, :, 0:15], rz.at[g])
            acc[...] = jnp.zeros_like(acc)

        at = g * 8 + (lax.broadcasted_iota(jnp.int32, (512, TILE), 0) & 7)
        own = (at >= SLOTS) == (e == 1)

        def step(f, _):
            n = STEPS + i * STEPS + f
            weights(n + 2)
            b = ready(n)
            rows = z[g].reshape(512, D)
            h = jax.nn.silu(dot(rows, bg[b])) * dot(rows, bu[b])
            acc[...] += dot(jnp.where(own, h, 0.0).astype(BF16), bd[b])
            return 0

        lax.fori_loop(0, STEPS, step, 0)

        @pl.when(i != 2)
        def _():
            z[g] = acc[...].astype(BF16).reshape(4, 4, 4, 8, D)
            give_back(g)

    def each(f):
        def run(i, _):
            f(i)
            return 0

        return run

    lax.fori_loop(1, GROUPS, each(dispatch), 0)
    lax.fori_loop(0, GROUPS + 1, each(experts), 0)

    for g in range(GROUPS):
        wait(back.at[:, g, 0:15], rc.at[g])
    def summed(p, i):
        mix = jnp.concatenate(
            [jnp.where(number == tables[p, i, g:g + 1, :], tables[p, i, 8 + g:9 + g, :], 0.0).astype(BF16)
             for g in range(GROUPS)], axis=1)
        return dot(mix, back[i, :, :, :, part(p)].reshape(GROUPS * 128, LANES[p][1]))

    for p in range(3):
        for k in range(2):
            wait(lines.at[0, HALF[0], part(p)], s1.at[p, 4 + k])
    for p in range(3):
        i = moved(p, 2)[p]
        lines[i, :, part(p)] = summed(p, i).astype(BF16)
        for k, by in enumerate((3, 1)):
            send(lines.at[i, HALF[k], part(p)], hop.at[k, :, part(p)], sl.at[p, k], rl.at[p, k], moved(p, by))
    for k, by in enumerate((3, 1)):
        for p in range(3):
            to = moved(p, by)
            own = summed(p, to[p])
            lines[to[p], HALF[1 - k], part(p)] = own[HALF[1 - k]].astype(BF16)
            send(lines.at[to[p], HALF[1 - k], part(p)], last.at[k, HALF[1 - k], part(p)],
                 sl.at[p, 2 + k], rl.at[p, 2 + k], to)
            acc[HALF[k], part(p)] = own[HALF[k]]
    for k, by in enumerate((3, 1)):
        for p in range(3):
            to = moved(p, by)
            wait(hop.at[k, :, part(p)], rl.at[p, k])
            both = acc[HALF[k], part(p)] + hop[k, :, part(p)].astype(F32)
            lines[to[p], HALF[k], part(p)] = both.astype(BF16)
            send(lines.at[to[p], HALF[k], part(p)], last.at[k, HALF[k], part(p)],
                 sl.at[p, 4 + k], rl.at[p, 4 + k], to)
    for p in range(3):
        total[:, part(p)] += summed(p, coord[p])
    for j in (2, 4):
        for k in range(2):
            half = HALF[1 - k] if j == 2 else HALF[k]
            for p in range(3):
                wait(last.at[k, half, part(p)], rl.at[p, j + k])
                both = total[half, part(p)] + last[k, half, part(p)].astype(F32)
                if j == 2:
                    total[half, part(p)] = both
                else:
                    y[half, part(p)] = both.astype(BF16)
                    pltpu.make_async_copy(y.at[half, part(p)], y_hbm.at[half, part(p)], ysem.at[k, p]).start()
    for k in range(2):
        for p in range(3):
            wait(y.at[HALF[k], part(p)], ysem.at[k, p])

    for p in range(3):
        for k in range(6):
            if k < 4:
                wait(lines.at[0, HALF[0], part(p)], s1.at[p, k])
            wait(lines.at[0, HALF[0], part(p)], sl.at[p, k])
        wait(tables.at[p, 0:3], st.at[p])
    for g in range(GROUPS):
        wait(out_rows.at[g, :, 0:15], sz.at[g])
        wait(back.at[:, g, 0:15], sc.at[g])


def solution(mesh):
    dma = pltpu.SemaphoreType.DMA

    def body(x, expert, slot, gate, wg, wu, wd, sg, su, sd):
        anywhere = pl.BlockSpec(memory_space=pl.ANY)
        out = pl.pallas_call(
            kernel,
            out_shape=jax.ShapeDtypeStruct((T, D), BF16),
            in_specs=[anywhere] * 10,
            out_specs=anywhere,
            scratch_shapes=[
                pltpu.VMEM((4, T, D), BF16),
                pltpu.VMEM((3, 4, 16, 128), F32),
                pltpu.VMEM((3, 4, 16, 128), F32),
                pltpu.VMEM((GROUPS, 4, 16, 8, D), BF16),
                pltpu.VMEM((GROUPS, 4, 4, 4, 8, D), BF16),
                pltpu.VMEM((4, GROUPS, 16, 8, D), BF16),
                pltpu.VMEM((512, D), F32),
                pltpu.VMEM((T, D), F32),
                pltpu.VMEM((2, T // 2, D), BF16),
                pltpu.VMEM((2, T, D), BF16),
                pltpu.VMEM((BUFS, D, TILE), BF16),
                pltpu.VMEM((BUFS, D, TILE), BF16),
                pltpu.VMEM((BUFS, TILE, D), BF16),
                dma((3, 6)), dma((3, 6)), dma((3,)), dma((3,)),
                dma((GROUPS,)), dma((GROUPS,)), dma((GROUPS,)), dma((GROUPS,)),
                dma((3, 6)), dma((3, 6)), dma((BUFS, 3)),
                pltpu.VMEM((T, D), BF16), dma(()),
                pltpu.VMEM((TOP, T), jnp.int32), pltpu.VMEM((TOP, T), jnp.int32), pltpu.VMEM((TOP, T), F32), dma((3,)),
                pltpu.VMEM((T, D), BF16), dma((2, 3)), pltpu.SemaphoreType.REGULAR,
            ],
            compiler_params=pltpu.CompilerParams(has_side_effects=True, collective_id=0, vmem_limit_bytes=67043328),
            name="moe",
        )(x[0, 0], expert[0, 0].T, slot[0, 0].T, gate[0, 0].T, wg, wu, wd, sg, su, sd)
        return out[None, None]

    tokens, experts = P("dp", "ep", None, None), P("ep", None, None)
    return jax.shard_map(body, mesh=mesh, in_specs=(tokens,) * 4 + (experts,) * 3 + (P(None, None),) * 3,
                         out_specs=tokens, check_vma=False)
```
